32 devices in a mesh: dp: 16 (over z, x, core), tensor: 2 (over y).
Axes of the slice: x: 2, y: 2, z: 4, core: 2. Of those that a mesh axis runs over, the one named last changes fastest.
Arguments:
- hidden: bfloat16 [5120, 18432], P('dp', 'tensor'), may hold values from -6 to 6
- fixed_down_weight: bfloat16 [18432, 4608], P('tensor', 'dp'), may hold values from -4 to 4
- lowrank_factor_b: bfloat16 [18432, 16], P('tensor'), may hold values from -0.046875 to 0.046875
- lowrank_factor_a: bfloat16 [16, 4608], P(None, 'dp'), may hold values from -1.5 to 1.5
- magnitude: float32 [4608], P('tensor'), may hold values from 0.5 to 2
- cotangent: bfloat16 [5120, 4608], P('dp', 'tensor'), may hold values from -0.083496094 to 0.083496094
Outputs:
- mixed: bfloat16 [5120, 4608], P('dp', 'tensor')
- gradient_column_scale: float32 [4608], P(('tensor', 'dp'))
- gradient_factor_a: float32 [16, 4608], P(None, ('tensor', 'dp'))
- gradient_factor_b: float32 [18432, 16], P(('tensor', 'dp'))
The draws below stay inside these ranges and needn't reach their ends.
All inputs are finite; a program needn't handle non-finite values.
Results may differ from the reference program's by a relative error of at most 0.0054.
Values may be sent and summed in bfloat16 or wider, within the bound.
A program may use at most 192 MiB of HBM per device.

```python
import math
import jax
import jax.numpy as jnp
from jax import lax

MODEL_WIDTH = 4608
HALF_FEEDFORWARD = 18432
ADAPTER_RANK = 16
TOK_DEV = 320
TOKENS = 5120
N_DP = 16


def draw_fixed_down_weight(key, part):
    base = jax.random.truncated_normal(key, -4.0, 4.0, (HALF_FEEDFORWARD, MODEL_WIDTH), jnp.float32) * HALF_FEEDFORWARD ** (-0.5)
    ramp = 0.5 + jnp.arange(HALF_FEEDFORWARD, dtype=jnp.float32) / (HALF_FEEDFORWARD - 1)
    return (base * ramp[:, None]).astype(jnp.bfloat16)


def raised(array, rng, source, target, shards_of, factor):
    owner, partner = [(jnp.arange(array.shape[dim]) // (array.shape[dim] // shards_of)).reshape([-1 if axis == dim else 1 for axis in range(array.ndim)]) for dim in (source, target)]
    chosen = jax.random.permutation(rng, shards_of)[partner]
    strong = (owner == chosen) | (owner == (partner + shards_of // 2) % shards_of)
    return jnp.where(strong, factor * array, array)


def levels(key, extent, shards, low, largest):
    factor_of = 1.0
    for axis_at, shards_of in shards:
        steps = jax.random.uniform(jax.random.fold_in(jax.random.fold_in(key, 6), axis_at), (shards_of,), jnp.float32, low / len(shards), largest / len(shards))
        factor_of = factor_of * jnp.repeat(jnp.exp(steps), extent[axis_at] // shards_of).reshape((-1,) + (1,) * (len(extent) - 1 - axis_at))
    return factor_of


def normal_values(rng, extent, deviation, limit, pieces=(), held_as=jnp.bfloat16):
    gain = levels(rng, extent, pieces, -0.22, 0.18) if pieces else 1.0
    values = jax.random.normal(rng, extent, jnp.float32) * deviation * gain
    return jnp.minimum(jnp.maximum(values, -limit), limit).astype(held_as)


def bell_draw_with(own_key, extent, spread, bound, cuts, heavy, held_as=jnp.bfloat16):
    array = spread * jax.random.normal(own_key, extent, jnp.float32)
    if cuts:
        array = array * levels(own_key, extent, cuts, -0.22, 0.18)
    return jnp.clip(raised(array, jax.random.fold_in(own_key, 3), *heavy), -bound, bound).astype(held_as)


def setup_inputs(seed: int = 0) -> dict:
    arg_keys = jax.random.split(jax.random.key(seed), 7)
    return {
        "hidden": bell_draw_with(arg_keys[0], (TOKENS, HALF_FEEDFORWARD), 1.0, 6.0, ((0, 16), (1, 2)), (0, 1, 16, 2.0)),
        "fixed_down_weight": draw_fixed_down_weight(jax.random.fold_in(arg_keys[6], 71), 0),
        "lowrank_factor_b": normal_values(arg_keys[2], (HALF_FEEDFORWARD, ADAPTER_RANK), HALF_FEEDFORWARD ** -0.5, 0.046875, ((0, 2),)),
        "lowrank_factor_a": normal_values(arg_keys[3], (ADAPTER_RANK, MODEL_WIDTH), ADAPTER_RANK ** -0.5, 1.5, ((1, 16),)),
        "magnitude": jnp.clip(jnp.exp(math.log(2.0) - 1.3862944 * jax.random.uniform(arg_keys[4], (MODEL_WIDTH,), jnp.float32) ** levels(arg_keys[4], (MODEL_WIDTH,), ((0, 2),), -0.2, 0.2)), 0.5, 2.0),
        "cotangent": bell_draw_with(arg_keys[5], (TOKENS, MODEL_WIDTH), ((TOK_DEV * N_DP) ** -0.5), 0.083496094, ((0, 16), (1, 2)), (0, 1, 16, 2.0)),
    }


def squared_column_entries(fixed_down_weight, lowrank_factor_b, lowrank_factor_a):
    w_blocks = fixed_down_weight.reshape(8, HALF_FEEDFORWARD // 8, MODEL_WIDTH)
    factor_b_blocks = lowrank_factor_b.reshape(8, HALF_FEEDFORWARD // 8, ADAPTER_RANK)

    def one_block(pair):
        weight_tile_block, factor_b_block = pair
        combined_weight = weight_tile_block.astype(jnp.float32) + jnp.dot(factor_b_block, lowrank_factor_a, preferred_element_type=jnp.float32)
        return lax.optimization_barrier(jnp.sum(combined_weight * combined_weight, axis=0))
    return lax.optimization_barrier(jnp.sum(lax.map(one_block, (w_blocks, factor_b_blocks)), axis=0))

def reference(hidden, fixed_down_weight, lowrank_factor_b, lowrank_factor_a, magnitude, cotangent):
    column_norm_values = jnp.sqrt(squared_column_entries(fixed_down_weight, lowrank_factor_b, lowrank_factor_a) + 1e-06)
    scale = magnitude / column_norm_values
    lowrank_update = jnp.dot(hidden, lowrank_factor_b, preferred_element_type=jnp.float32)
    lowrank_block_update = lowrank_update.astype(jnp.bfloat16)
    prenorm_output = jnp.dot(hidden, fixed_down_weight, preferred_element_type=jnp.float32) + jnp.dot(lowrank_block_update, lowrank_factor_a, preferred_element_type=jnp.float32)
    mixed = (prenorm_output * scale).astype(jnp.bfloat16)
    cot = cotangent.astype(jnp.float32)
    gradient_column_scale = lax.optimization_barrier(jnp.sum(cot * prenorm_output, axis=0)) / column_norm_values
    prenorm_gradient_b = (cot * scale).astype(jnp.bfloat16)
    gradient_factor_a = jnp.dot(lowrank_block_update.T, prenorm_gradient_b, preferred_element_type=jnp.float32)
    backward_factor_b = jnp.dot(prenorm_gradient_b, lowrank_factor_a.T, preferred_element_type=jnp.float32).astype(jnp.bfloat16)
    gradient_factor_b = jnp.dot(hidden.T, backward_factor_b, preferred_element_type=jnp.float32)
    return (mixed, gradient_column_scale, gradient_factor_a, gradient_factor_b)
```

```python
import jax
import jax.numpy as jnp
from jax import lax
from jax.sharding import Mesh, PartitionSpec as P

F32, BF16 = jnp.float32, jnp.bfloat16


def body(hidden, weight, factor_b, factor_a, magnitude, cotangent, *, n_out, n_in, n_t):
    rows, depth = hidden.shape
    cols = weight.shape[1]
    rank = factor_b.shape[1]
    out_cols = magnitude.shape[0]
    group = 2 * n_in
    dp = ("outer", "mid", "core")
    outer = lax.axis_index("outer")
    place = lax.axis_index("mid") * 2 + lax.axis_index("core")
    own = lax.axis_index("tensor")

    swap_mid = [(i, (i + 1) % n_in) for i in range(n_in)]
    swap_core = [(0, 1), (1, 0)]
    h_mid = lax.ppermute(hidden, "mid", swap_mid)
    w_all = lax.all_gather(weight, "outer", axis=1, tiled=True)
    h_core = lax.ppermute(hidden, "core", swap_core)
    h_both = lax.ppermute(h_mid, "core", swap_core)

    low_part = jnp.dot(hidden, factor_b, preferred_element_type=F32)
    merged = weight.astype(F32) + jnp.dot(factor_b, factor_a, preferred_element_type=F32)
    local_sq = jnp.sum(merged * merged, axis=0)
    low, block_sq = lax.psum((low_part, local_sq), "tensor")
    col_sq = lax.all_gather(block_sq, dp, axis=0, tiled=True)
    full_a = lax.all_gather(factor_a, dp, axis=1, tiled=True)
    norms = jnp.sqrt(lax.dynamic_slice_in_dim(col_sq, own * out_cols, out_cols, 0) + 1e-06)
    scale = magnitude / norms
    low_b = low.astype(BF16)
    own_a = lax.dynamic_slice_in_dim(full_a, own * out_cols, out_cols, 1)
    adapter = jnp.dot(low_b, own_a, preferred_element_type=F32)

    h_all = jnp.zeros((group, rows, depth), BF16)
    for block, flip in ((hidden, 0), (h_core, 1), (h_mid, 2), (h_both, 3)):
        h_all = lax.dynamic_update_slice_in_dim(h_all, block[None], place ^ flip, 0)
    h_rows = h_all.reshape(group * rows, depth)

    cot = cotangent.astype(F32)
    dpre_b = (cot * scale).astype(BF16)
    back_b = lax.psum(jnp.dot(dpre_b, own_a.T, preferred_element_type=F32), "tensor").astype(BF16)
    b_part = jnp.dot(back_b.T, hidden, preferred_element_type=F32)
    a_part = jnp.dot(low_b.T, dpre_b, preferred_element_type=F32)
    n_dp = n_out * group
    parts = jnp.concatenate([x.reshape(rank, n_dp, -1) for x in (a_part, b_part)], axis=2)
    parts = lax.all_to_all(parts.transpose(1, 0, 2), dp, 0, 0, tiled=True)
    sums = jnp.sum(parts, axis=0)
    grad_a = sums[:, : out_cols // n_dp]
    grad_b = sums[:, out_cols // n_dp :].T
    w_all, grad_a, grad_b = lax.optimization_barrier((w_all, grad_a, grad_b))

    per_t = n_out // n_t
    sends = jnp.dot(h_rows, w_all, preferred_element_type=F32).astype(BF16)
    sends = sends.reshape(group, rows, n_t, per_t, cols).transpose(2, 0, 3, 1, 4)
    sends = sends.reshape(n_t * group, per_t, rows, cols)
    got = lax.all_to_all(sends, ("tensor", "mid", "core"), 0, 0, tiled=True)
    got = got.reshape(n_t, group, per_t, rows, cols)
    summed = jnp.sum(got.astype(F32), axis=0).transpose(2, 1, 0, 3).reshape(rows, out_cols)

    pre = summed + adapter
    mixed = (pre * scale).astype(BF16)
    mag_part = jnp.sum(cot * pre, axis=0) / norms
    for axis in ("core", "mid", "outer"):
        mag_part = lax.psum(mag_part, axis)
    at = (outer * group + place) * (out_cols // n_dp)
    grad_scale = lax.dynamic_slice_in_dim(mag_part, at, out_cols // n_dp, 0)
    return mixed, grad_scale, grad_a, grad_b


def solution(mesh):
    n_dp, n_t = mesh.shape["dp"], mesh.shape["tensor"]
    n_in = 2
    n_out = n_dp // (2 * n_in)
    fine = Mesh(mesh.devices.reshape(n_out, n_in, 2, n_t), ("outer", "mid", "core", "tensor"))
    dp = ("outer", "mid", "core")

    def step(*args):
        return body(*args, n_out=n_out, n_in=n_in, n_t=n_t)

    return jax.shard_map(
        step,
        mesh=fine,
        in_specs=(
            P(dp, "tensor"),
            P("tensor", dp),
            P("tensor", None),
            P(None, dp),
            P("tensor"),
            P(dp, "tensor"),
        ),
        out_specs=(
            P(dp, "tensor"),
            P(("tensor",) + dp),
            P(None, ("tensor",) + dp),
            P(("tensor",) + dp, None),
        ),
        check_vma=False,
    )
```
